512 devices in a mesh: wide: 32 (over x, y, core), narrow: 16 (over z).
Axes of the slice: x: 4, y: 4, z: 16, core: 2. Of those that a mesh axis runs over, the one named last changes fastest.
Arguments:
- samples: float32 [256, 65536], P('narrow', 'wide'), may hold values from -6 to 6
- row_weights: float32 [32768], P('narrow'), may hold values from 0.1 to 10
- tile_ranks: int32 [64, 128], P('narrow', 'wide'), may hold values from 16 to 80, as said below
- u_factors: bfloat16 [64, 128, 80, 512], P('narrow', 'wide'), may hold values from -0.078125 to 0.078125
- v_factors: bfloat16 [64, 128, 80, 512], P('narrow', 'wide'), may hold values from -0.25 to 0.25
Outputs:
- forward_rows: float32 [256, 32768], P('wide', 'narrow')
- adjoint_cols: float32 [256, 65536], P(None, ('wide', 'narrow'))
The draws below stay inside these ranges and needn't reach their ends.
Inputs may be any that keep to these rules, and one draw needn't show every extreme that they name: `tile_ranks`: every rank is a multiple of 16.
All inputs are finite; a program needn't handle non-finite values.
Results may differ from the reference program's by a relative error of at most 0.0085.
Values may be sent and summed in bfloat16 or wider, within the bound.
No kernel may reach another device: no remote copies, remote signals or barrier semaphores. Data moves between devices by JAX's collectives and lax.ppermute only.
A program may use at most 64 MiB of HBM per device.

```python
import math
import jax
import jax.numpy as jnp
from jax import lax

B = 512
RMAX = 80
S = 256
TILE_ROWS = 64
TILE_COLS = 128
ORDER_ROWS = 32768
ORDER_COLS = 65536


def draw_tile_ranks(key, part):
    steps = RMAX // 16
    base = jax.random.randint(jax.random.fold_in(key, 11), (TILE_ROWS, TILE_COLS), 1, steps + 1)
    offset = jax.random.randint(jax.random.fold_in(key, 13), (), 0, TILE_COLS)
    row_ids = jnp.arange(TILE_ROWS, dtype=jnp.int32)[:, None]
    col_ids = jnp.arange(TILE_COLS, dtype=jnp.int32)[None, :]
    centre = (row_ids * TILE_COLS // TILE_ROWS + offset) % TILE_COLS
    apart = (col_ids - centre) % TILE_COLS
    near_band = (apart <= 1) | (apart >= TILE_COLS - 1)
    levels = jnp.where(near_band, steps, base)
    lowest_col = (offset + TILE_COLS // 2) % TILE_COLS
    lowest = (row_ids == 0) & (col_ids == lowest_col)
    levels = jnp.where(lowest, 1, levels)
    return (16 * levels).astype(jnp.int32)


def level_of(own_key, extent, cuts, smallest, top_value):
    level, own = 1.0, jax.random.fold_in(own_key, 6)
    for axis_at, blocks in cuts:
        draws = jnp.exp(jax.random.uniform(jax.random.fold_in(own, axis_at), (blocks,), jnp.float32, smallest / len(cuts), top_value / len(cuts)))
        level = level * jnp.repeat(draws, extent[axis_at] // blocks).reshape([-1 if axis == axis_at else 1 for axis in range(len(extent))])
    return level


def noise(rng, shape, scale, reach, pieces=(), kind=jnp.bfloat16):
    result = jax.random.normal(rng, shape, jnp.float32) * scale
    if len(pieces) > 0:
        result = level_of(rng, shape, pieces, -0.22, 0.18) * result
    return jnp.clip(result, min=-reach, max=reach).astype(kind)


def setup_inputs(seed: int = 0) -> dict:
    arg_keys = jax.random.split(jax.random.key(seed), 6)
    return {
        "samples": noise(arg_keys[0], (S, ORDER_COLS), 1.0, 6.0, ((0, 16), (1, 32)), jnp.float32),
        "row_weights": jnp.clip(jnp.exp(math.log(10.0) - 4.6051702 * jax.random.uniform(arg_keys[1], (ORDER_ROWS,), jnp.float32) ** level_of(arg_keys[1], (ORDER_ROWS,), ((0, 16),), -0.2, 0.2)), 0.1, 10.0),
        "tile_ranks": draw_tile_ranks(jax.random.fold_in(arg_keys[5], 71), 0),
        "u_factors": noise(arg_keys[3], (TILE_ROWS, TILE_COLS, RMAX, B), (RMAX * TILE_COLS // 2) ** -0.5, 0.078125, ((0, 16), (1, 32))),
        "v_factors": noise(arg_keys[4], (TILE_ROWS, TILE_COLS, RMAX, B), B ** -0.5, 0.25, ((0, 16), (1, 32))),
    }


def reference(samples, row_weights, tile_ranks, u_factors, v_factors):
    tile_rows, tile_cols, rank_cap, tile_size = v_factors.shape
    col_count = samples.shape[0]
    levels = jnp.arange(rank_cap, dtype=jnp.int32)
    rank_mask = (levels[None, None, :] < tile_ranks[:, :, None]).astype(jnp.float32)
    columns = samples.astype(jnp.bfloat16).astype(jnp.float32).reshape(col_count, tile_cols, tile_size)
    highest = lax.Precision.HIGHEST

    def forward(tile_index):
        v_block = lax.dynamic_index_in_dim(v_factors, tile_index, 0, keepdims=False).astype(jnp.float32)
        u_block = lax.dynamic_index_in_dim(u_factors, tile_index, 0, keepdims=False).astype(jnp.float32)
        row_mask = lax.dynamic_index_in_dim(rank_mask, tile_index, 0, keepdims=False)
        coeffs = jnp.einsum("sjb,jrb->jrs", columns, v_block, precision=highest) * row_mask[:, :, None]
        coeffs = coeffs.astype(jnp.bfloat16).astype(jnp.float32)
        return jnp.einsum("jrs,jrb->sb", coeffs, u_block, precision=highest)

    row_blocks = lax.map(forward, jnp.arange(tile_rows, dtype=jnp.int32))
    row_total = jnp.transpose(row_blocks, (1, 0, 2)).reshape(col_count, tile_rows * tile_size)
    weighted = (row_total * row_weights[None, :]).astype(jnp.bfloat16).astype(jnp.float32)
    weighted = weighted.reshape(col_count, tile_rows, tile_size)

    def adjoint(tile_index):
        u_block = lax.dynamic_index_in_dim(u_factors, tile_index, 1, keepdims=False).astype(jnp.float32)
        v_block = lax.dynamic_index_in_dim(v_factors, tile_index, 1, keepdims=False).astype(jnp.float32)
        col_mask = lax.dynamic_index_in_dim(rank_mask, tile_index, 1, keepdims=False)
        adjoint_coeffs = jnp.einsum("sib,irb->irs", weighted, u_block, precision=highest) * col_mask[:, :, None]
        adjoint_coeffs = adjoint_coeffs.astype(jnp.bfloat16).astype(jnp.float32)
        return jnp.einsum("irs,irb->sb", adjoint_coeffs, v_block, precision=highest)

    col_blocks = lax.map(adjoint, jnp.arange(tile_cols, dtype=jnp.int32))
    col_total = jnp.transpose(col_blocks, (1, 0, 2)).reshape(col_count, tile_cols * tile_size)
    return row_total, col_total
```

```python
import functools

import jax
import jax.numpy as jnp
from jax import lax
from jax.experimental import pallas as pl
from jax.experimental.pallas import tpu as pltpu
from jax.sharding import Mesh
from jax.sharding import PartitionSpec as P

LINE = ("zh", "zl")
PAIR_LINE = ("c", "zh", "zl")
NT = (((1,), (1,)), ((), ()))
TN = (((0,), (0,)), ((), ()))


def turned(steps):
    return [
        (c * 16 + z, c * 16 + (z + (steps if c == 0 else -steps)) % 16)
        for c in range(2)
        for z in range(16)
    ]


def forward_kernel(at, own, one, two, low, high, v0, v1, u0, u1, out, coeffs):
    core = at[0]
    for k, v in enumerate((v0, v1)):
        side = jnp.bitwise_xor(core, k)
        for j in range(4):
            cols = pl.ds(j * 512, 512)
            x = jnp.concatenate([piece[side, :, cols] for piece in (own, one, two, low, high)], 0)
            tall = jnp.concatenate([v[i, j] for i in range(4)], 0)
            c = lax.dot_general(tall, x, NT, preferred_element_type=jnp.float32)
            for i in range(4):
                coeffs[i, pl.ds(k * 320 + j * 80, 80), :] = c[i * 80 : i * 80 + 80].astype(jnp.bfloat16)
    for i in range(4):
        u = jnp.concatenate([u[i, j] for u in (u0, u1) for j in range(4)], 0)
        part = lax.dot_general(coeffs[i], u, TN, preferred_element_type=jnp.float32)
        for p in range(4):
            for zh in range(4):
                row = p * 32 + zh * 8
                out[zh * 4 + at[1 + p], :, pl.ds(i * 512, 512)] = part[row : row + 8].astype(jnp.bfloat16)


def adjoint_kernel(at, w, v0, v1, u0, u1, own, one, two, low, high, coeffs, blocks):
    core = at[0]
    for k, u in enumerate((u0, u1)):
        for i in range(4):
            tall = jnp.concatenate([u[i, j] for j in range(4)], 0)
            a = lax.dot_general(tall, w[:, pl.ds(i * 512, 512)], NT, preferred_element_type=jnp.float32)
            for j in range(4):
                coeffs[k, j, pl.ds(i * 80, 80), :] = a[j * 80 : j * 80 + 80].astype(jnp.bfloat16)
    for k, v in enumerate((v0, v1)):
        side = jnp.bitwise_xor(core, k)
        for j in range(4):
            tall = jnp.concatenate([v[i, j] for i in range(4)], 0)
            back = lax.dot_general(coeffs[k, j], tall, TN, preferred_element_type=jnp.float32)
            back = back.astype(jnp.bfloat16)
            for q in range(4):
                blocks[q, side, j] = back[:, q * 128 : q * 128 + 128]
    own[...] = blocks[at[1]]
    one[...] = blocks[at[2]]
    two[...] = blocks[at[3]]
    low[...] = blocks[at[4], :, :2]
    high[...] = blocks[at[4], :, 2:]


SMEM = pl.BlockSpec(memory_space=pltpu.SMEM)
VMEM = pl.BlockSpec(memory_space=pltpu.VMEM)


def forward_part(at, pieces, v, u):
    return pl.pallas_call(
        forward_kernel,
        out_shape=jax.ShapeDtypeStruct((16, 8, 2048), jnp.bfloat16),
        in_specs=[SMEM] + [VMEM] * 9,
        out_specs=VMEM,
        scratch_shapes=[pltpu.VMEM((4, 640, 128), jnp.bfloat16)],
        name="forward_part",
    )(at, *pieces, *v, *u)


def adjoint_part(at, weighted, v, u):
    full = jax.ShapeDtypeStruct((2, 4, 128, 128), jnp.bfloat16)
    half = jax.ShapeDtypeStruct((2, 2, 128, 128), jnp.bfloat16)
    return pl.pallas_call(
        adjoint_kernel,
        out_shape=(full, full, full, half, half),
        in_specs=[SMEM] + [VMEM] * 5,
        out_specs=(VMEM,) * 5,
        scratch_shapes=[
            pltpu.VMEM((2, 4, 320, 128), jnp.bfloat16),
            pltpu.VMEM((4, 2, 4, 128, 128), jnp.bfloat16),
        ],
        name="adjoint_part",
    )(at, weighted, *v, *u)


def exchange(blocks, axes):
    return lax.all_to_all(blocks, axes, split_axis=0, concat_axis=0, tiled=True)


def to_neighbours(own, one, two, low, high):
    del own
    got_one = lax.ppermute(one, PAIR_LINE, turned(1))
    got_two = lax.ppermute(two, PAIR_LINE, turned(-1))
    got_low = lax.ppermute(low, PAIR_LINE, turned(2))
    got_high = lax.ppermute(high, PAIR_LINE, turned(-2))
    return got_one, got_two, got_low, got_high


def on_device(samples, row_weights, tile_ranks, u_factors, v_factors):
    core = lax.axis_index("c")
    place = lax.axis_index("zl")
    turn = 1 - 2 * core
    swap = functools.partial(lax.ppermute, axis_name="c", perm=[(0, 1), (1, 0)])

    x = samples.astype(jnp.bfloat16).reshape(2, 1, 8, 2048)
    x = jnp.broadcast_to(x, (2, 4, 8, 2048)).reshape(8, 8, 2048)
    far = exchange(x, ("c", "zh")).reshape(2, 32, 2048)
    v = (v_factors, swap(v_factors))
    levels = lax.broadcasted_iota(jnp.int32, (1, 1, 80, 1), 2)
    kept = jnp.where(levels < tile_ranks[:, :, None, None], u_factors, jnp.zeros_like(u_factors))
    u = (kept, swap(kept))

    one, two, low, high = to_neighbours(far, far, far, far[:, :16], far[:, 16:])
    at = jnp.stack([core, place, (place - turn) % 4, (place + turn) % 4, (place + 2) % 4]).astype(jnp.int32)
    part = forward_part(at, (far, one, two, low, high), v, u)
    forward_rows = jnp.sum(exchange(part, ("xy",)).astype(jnp.float32), axis=0)

    weighted = (forward_rows * row_weights[None, :]).astype(jnp.bfloat16)
    weighted = exchange(jnp.broadcast_to(weighted, (16, 8, 2048)), ("xy",)).reshape(128, 2048)

    to = jnp.stack([core, place, (place + turn) % 4, (place - turn) % 4, (place + 2) % 4]).astype(jnp.int32)
    blocks = adjoint_part(to, weighted, v, u)
    one, two, low, high = to_neighbours(*blocks)
    wide = lambda b: b.astype(jnp.float32)
    near = wide(blocks[0]) + wide(one) + wide(two) + wide(jnp.concatenate([low, high], 1))
    near = near.astype(jnp.bfloat16).reshape(8, 128, 128)
    back = exchange(near, ("c", "zh")).reshape(2, 4, 16, 8, 128)
    back = jnp.sum(back.astype(jnp.float32), axis=1)
    adjoint_cols = jnp.swapaxes(back, 0, 1).reshape(256, 128)
    return forward_rows, adjoint_cols


def solution(mesh):
    fine = Mesh(mesh.devices.reshape(16, 2, 4, 4), ("xy", "c", "zh", "zl"))
    narrow, wide = LINE, ("xy", "c")
    in_specs = (
        P(narrow, wide),
        P(narrow),
        P(narrow, wide),
        P(narrow, wide, None, None),
        P(narrow, wide, None, None),
    )
    out_specs = (P(wide, narrow), P(None, (*wide, *narrow)))
    return jax.shard_map(on_device, mesh=fine, in_specs=in_specs, out_specs=out_specs, check_vma=False)
```

```python
import functools

import jax
import jax.numpy as jnp
from jax import lax
from jax.experimental import pallas as pl
from jax.experimental.pallas import tpu as pltpu
from jax.sharding import Mesh
from jax.sharding import PartitionSpec as P

LINE = ("zh", "zl")
PAIR_LINE = ("c", "zh", "zl")
NT = (((1,), (1,)), ((), ()))
TN = (((0,), (0,)), ((), ()))
STEPS = (0, -5, 5, -1, -6, 4, 1, -4, 6, -2, -7, 3, 2, -3, 7, -8)


def turned(x, steps):
    pairs = [
        (c * 16 + z, c * 16 + (z + (steps if c == 0 else -steps)) % 16)
        for c in range(2)
        for z in range(16)
    ]
    return lax.ppermute(x, PAIR_LINE, pairs)


def forward_kernel(home, p0, p1, p2, p3, p4, p5, v0, v1, u0, u1, out, x, coeffs):
    for s in range(16):
        block = p5 if s == 15 else (p0, p1, p2, p3, p4)[s // 3].at[s % 3]
        for k in range(2):
            x[k, home[s]] = block[k]
    for k, v in enumerate((v0, v1)):
        for j in range(4):
            xj = x[k, :, :, pl.ds(j * 512, 512)].reshape(128, 512)
            tall = jnp.concatenate([v[i, j] for i in range(4)], 0)
            c = lax.dot_general(tall, xj, NT, preferred_element_type=jnp.float32)
            for i in range(4):
                coeffs[i, pl.ds(k * 320 + j * 80, 80), :] = c[i * 80 : i * 80 + 80].astype(jnp.bfloat16)
    for i in range(4):
        u = jnp.concatenate([u[i, j] for u in (u0, u1) for j in range(4)], 0)
        part = lax.dot_general(coeffs[i], u, TN, preferred_element_type=jnp.float32)
        out[:, :, pl.ds(i * 512, 512)] = part.reshape(16, 8, 512).astype(jnp.bfloat16)


def adjoint_kernel(home, w, v0, v1, u0, u1, p0, p1, p2, p3, p4, p5, coeffs, blocks):
    for k, u in enumerate((u0, u1)):
        for i in range(4):
            tall = jnp.concatenate([u[i, j] for j in range(4)], 0)
            a = lax.dot_general(tall, w[:, pl.ds(i * 512, 512)], NT, preferred_element_type=jnp.float32)
            for j in range(4):
                coeffs[k, j, pl.ds(i * 80, 80), :] = a[j * 80 : j * 80 + 80].astype(jnp.bfloat16)
    for k, v in enumerate((v0, v1)):
        for j in range(4):
            tall = jnp.concatenate([v[i, j] for i in range(4)], 0)
            back = lax.dot_general(coeffs[k, j], tall, TN, preferred_element_type=jnp.float32)
            back = back.astype(jnp.bfloat16)
            for q in range(4):
                blocks[4 * j + q, k] = back[:, q * 128 : q * 128 + 128]
    for s in range(16):
        block = p5 if s == 15 else (p0, p1, p2, p3, p4)[s // 3].at[s % 3]
        block[...] = blocks[home[s]]


SMEM = pl.BlockSpec(memory_space=pltpu.SMEM)
VMEM = pl.BlockSpec(memory_space=pltpu.VMEM)
ROOM = pltpu.CompilerParams(vmem_limit_bytes=20 * 1024 * 1024)


def forward_part(home, pieces, v, u):
    return pl.pallas_call(
        forward_kernel,
        out_shape=jax.ShapeDtypeStruct((16, 8, 2048), jnp.bfloat16),
        in_specs=[SMEM] + [VMEM] * 10,
        out_specs=VMEM,
        scratch_shapes=[
            pltpu.VMEM((2, 16, 8, 2048), jnp.bfloat16),
            pltpu.VMEM((4, 640, 128), jnp.bfloat16),
        ],
        compiler_params=ROOM,
        name="forward_part",
    )(home, *pieces, *v, *u)


def adjoint_part(home, weighted, v, u):
    three = jax.ShapeDtypeStruct((3, 2, 128, 128), jnp.bfloat16)
    single = jax.ShapeDtypeStruct((2, 128, 128), jnp.bfloat16)
    return pl.pallas_call(
        adjoint_kernel,
        out_shape=(three,) * 5 + (single,),
        in_specs=[SMEM] + [VMEM] * 5,
        out_specs=(VMEM,) * 6,
        scratch_shapes=[
            pltpu.VMEM((2, 4, 320, 128), jnp.bfloat16),
            pltpu.VMEM((16, 2, 128, 128), jnp.bfloat16),
        ],
        compiler_params=ROOM,
        name="adjoint_part",
    )(home, weighted, *v, *u)


def exchange(blocks, axes):
    return lax.all_to_all(blocks, axes, split_axis=0, concat_axis=0, tiled=True)


def line_gather(block):
    back = turned(block, 5)
    ahead = turned(block, -5)
    three = jnp.stack([block, back, ahead])
    return (
        three,
        turned(three, 1),
        turned(three, -1),
        turned(three, 2),
        turned(three, -2),
        turned(back, 3),
    )


def line_sum(p0, p1, p2, p3, p4, p5):
    near = [turned(p1, -1), turned(p2, 1), turned(p3, -2), turned(p4, 2)]
    half_way = turned(p5, -3)
    total = p0.astype(jnp.float32)
    for blocks in near:
        total = total + blocks.astype(jnp.float32)
    behind = (total[1] + half_way.astype(jnp.float32)).astype(jnp.bfloat16)
    ahead = total[2].astype(jnp.bfloat16)
    own = total[0]
    return own + turned(behind, -5).astype(jnp.float32) + turned(ahead, 5).astype(jnp.float32)


def both_products(samples, row_weights, tile_ranks, u_factors, v_factors):
    core = lax.axis_index("c")
    swap = functools.partial(lax.ppermute, axis_name="c", perm=[(0, 1), (1, 0)])
    home = (lax.axis_index(LINE) + (1 - 2 * core) * jnp.array(STEPS, jnp.int32)) & 15

    x = samples.astype(jnp.bfloat16).reshape(2, 8, 2048)
    kept = lax.dynamic_index_in_dim(x, core, 0, keepdims=False)
    given = lax.dynamic_index_in_dim(x, 1 - core, 0, keepdims=False)
    block = jnp.stack([kept, swap(given)])
    block, u_factors, v_factors = lax.optimization_barrier((block, u_factors, v_factors))
    pieces = line_gather(block)
    levels = lax.broadcasted_iota(jnp.int32, (1, 1, 80, 1), 2)
    ranked = jnp.where(levels < tile_ranks[:, :, None, None], u_factors, jnp.zeros_like(u_factors))
    v = (v_factors, swap(v_factors))
    u = (ranked, swap(ranked))

    part = forward_part(home, pieces, v, u)
    forward_rows = jnp.sum(exchange(part, ("xy",)).astype(jnp.float32), axis=0)

    weighted = (forward_rows * row_weights[None, :]).astype(jnp.bfloat16)
    weighted = exchange(jnp.broadcast_to(weighted, (16, 8, 2048)), ("xy",)).reshape(128, 2048)

    own, other = line_sum(*adjoint_part(home, weighted, v, u))
    got = swap(other)
    even = jnp.where(core == 0, own, got).reshape(16, 1, 8, 128)
    odd = jnp.where(core == 0, got, own).reshape(16, 1, 8, 128)
    adjoint_cols = jnp.concatenate([even, odd], 1).reshape(256, 128)
    return forward_rows, adjoint_cols


def solution(mesh):
    fine = Mesh(mesh.devices.reshape(16, 2, 4, 4), ("xy", "c", "zh", "zl"))
    narrow, wide = LINE, ("xy", "c")
    in_specs = (
        P(narrow, wide),
        P(narrow),
        P(narrow, wide),
        P(narrow, wide, None, None),
        P(narrow, wide, None, None),
    )
    out_specs = (P(wide, narrow), P(None, (*wide, *narrow)))
    return jax.shard_map(both_products, mesh=fine, in_specs=in_specs, out_specs=out_specs, check_vma=False)
```

```python
import functools

import jax
import jax.numpy as jnp
from jax import lax
from jax.experimental import pallas as pl
from jax.experimental.pallas import tpu as pltpu
from jax.sharding import Mesh
from jax.sharding import PartitionSpec as P

LINE = ("zh", "zl")
PAIR_LINE = ("c", "zh", "zl")
NT = (((1,), (1,)), ((), ()))
TN = (((0,), (0,)), ((), ()))
MAIN = 1920


def turned(x, steps):
    pairs = [
        (c * 16 + z, c * 16 + (z + (steps if c == 0 else -steps)) % 16)
        for c in range(2)
        for z in range(16)
    ]
    return lax.ppermute(x, PAIR_LINE, pairs)


def forward_kernel(core, ranks, main, rest, v, u, mine, theirs, coeffs):
    for j in range(4):
        if j < 3:
            x = main[:, pl.ds(j * 512, 512)]
        else:
            x = jnp.concatenate([main[:, pl.ds(1536, MAIN - 1536)], rest[...]], 1)
        tall = jnp.concatenate([v[i, j] for i in range(4)], 0)
        c = lax.dot_general(tall, x, NT, preferred_element_type=jnp.float32)
        for i in range(4):
            part = c[i * 80 : i * 80 + 80]
            level = lax.broadcasted_iota(jnp.int32, part.shape, 0)
            part = jnp.where(level < ranks[i, j], part, 0.0)
            coeffs[i, pl.ds(j * 80, 80), :] = part.astype(jnp.bfloat16)
    for i in range(4):
        tall = jnp.concatenate([u[i, j] for j in range(4)], 0)
        part = lax.dot_general(coeffs[i], tall, TN, preferred_element_type=jnp.float32)
        part = part.reshape(16, 2, 8, 512)
        first = core[0] == 0
        cols = pl.ds(i * 512, 512)
        mine[:, :, cols] = jnp.where(first, part[:, 0], part[:, 1])
        theirs[:, :, cols] = jnp.where(first, part[:, 1], part[:, 0]).astype(jnp.bfloat16)


def adjoint_kernel(at, w, v0, v1, u0, u1, own, one, two, three, coeffs, blocks):
    for k, u in enumerate((u0, u1)):
        for i in range(4):
            tall = jnp.concatenate([u[i, j] for j in range(4)], 0)
            a = lax.dot_general(tall, w[:, pl.ds(i * 512, 512)], NT, preferred_element_type=jnp.float32)
            for j in range(4):
                coeffs[k, j, pl.ds(i * 80, 80), :] = a[j * 80 : j * 80 + 80].astype(jnp.bfloat16)
    for k, v in enumerate((v0, v1)):
        side = jnp.bitwise_xor(at[0], k)
        for j in range(4):
            tall = jnp.concatenate([v[i, j] for i in range(4)], 0)
            back = lax.dot_general(coeffs[k, j], tall, TN, preferred_element_type=jnp.float32)
            back = back.astype(jnp.bfloat16)
            for q in range(4):
                blocks[q, side, j] = back[:, q * 128 : q * 128 + 128]
    own[...] = blocks[at[1]]
    one[...] = blocks[at[2]]
    two[...] = blocks[at[3]]
    three[...] = blocks[at[4]]


SMEM = pl.BlockSpec(memory_space=pltpu.SMEM)
VMEM = pl.BlockSpec(memory_space=pltpu.VMEM)
ROOM = pltpu.CompilerParams(vmem_limit_bytes=20 * 1024 * 1024)


def forward_part(core, ranks, main, rest, v, u):
    return pl.pallas_call(
        forward_kernel,
        out_shape=(
            jax.ShapeDtypeStruct((16, 8, 2048), jnp.float32),
            jax.ShapeDtypeStruct((16, 8, 2048), jnp.bfloat16),
        ),
        in_specs=[SMEM, SMEM] + [VMEM] * 4,
        out_specs=(VMEM, VMEM),
        scratch_shapes=[pltpu.VMEM((4, 320, 256), jnp.bfloat16)],
        compiler_params=ROOM,
        name="forward_part",
    )(core, ranks, main, rest, v, u)


def adjoint_part(at, weighted, v, u):
    blocks = jax.ShapeDtypeStruct((2, 4, 128, 128), jnp.bfloat16)
    return pl.pallas_call(
        adjoint_kernel,
        out_shape=(blocks,) * 4,
        in_specs=[SMEM] + [VMEM] * 5,
        out_specs=(VMEM,) * 4,
        scratch_shapes=[
            pltpu.VMEM((2, 4, 320, 128), jnp.bfloat16),
            pltpu.VMEM((4, 2, 4, 128, 128), jnp.bfloat16),
        ],
        compiler_params=ROOM,
        name="adjoint_part",
    )(at, weighted, *v, *u)


def exchange(blocks, axes):
    return lax.all_to_all(blocks, axes, split_axis=0, concat_axis=0, tiled=True)


def wide(x):
    return x.astype(jnp.float32)


def both_products(samples, row_weights, tile_ranks, u_factors, v_factors):
    core = lax.axis_index("c")
    place = lax.axis_index("zl")
    turn = 1 - 2 * core
    swap = functools.partial(lax.ppermute, axis_name="c", perm=[(0, 1), (1, 0)])

    x = samples.astype(jnp.bfloat16)
    rest = exchange(jnp.broadcast_to(x[:, MAIN:], (16, 16, 2048 - MAIN)), LINE).reshape(256, -1)
    main = lax.all_gather(x[:, :MAIN], LINE, axis=0, tiled=True)
    mine, theirs = forward_part(core[None].astype(jnp.int32), tile_ranks, main, rest, v_factors, u_factors)
    part = (mine + wide(swap(theirs))).astype(jnp.bfloat16)
    forward_rows = jnp.sum(wide(exchange(part, ("xy",))), axis=0)

    weighted = (forward_rows * row_weights[None, :]).astype(jnp.bfloat16)
    weighted, u_factors, v_factors = lax.optimization_barrier((weighted, u_factors, v_factors))
    weighted = exchange(jnp.broadcast_to(weighted, (16, 8, 2048)), ("xy",)).reshape(128, 2048)
    levels = lax.broadcasted_iota(jnp.int32, (1, 1, 80, 1), 2)
    ranked = jnp.where(levels < tile_ranks[:, :, None, None], u_factors, jnp.zeros_like(u_factors))
    v = (v_factors, swap(v_factors))
    u = (ranked, swap(ranked))

    at = jnp.stack([core, place, (place + turn) & 3, (place - turn) & 3, (place + 2) & 3]).astype(jnp.int32)
    own, one, two, three = adjoint_part(at, weighted, v, u)
    near = wide(own) + wide(turned(one, 1)) + wide(turned(two, -1)) + wide(turned(three, 2))
    near = near.astype(jnp.bfloat16).reshape(8, 128, 128)
    back = exchange(near, ("c", "zh")).reshape(2, 4, 16, 8, 128)
    back = jnp.sum(wide(back), axis=1)
    adjoint_cols = jnp.swapaxes(back, 0, 1).reshape(256, 128)
    return forward_rows, adjoint_cols


def solution(mesh):
    fine = Mesh(mesh.devices.reshape(16, 2, 4, 4), ("xy", "c", "zh", "zl"))
    narrow, wide_axes = LINE, ("xy", "c")
    in_specs = (
        P(narrow, wide_axes),
        P(narrow),
        P(narrow, wide_axes),
        P(narrow, wide_axes, None, None),
        P(narrow, wide_axes, None, None),
    )
    out_specs = (P(wide_axes, narrow), P(None, (*wide_axes, *narrow)))
    return jax.shard_map(both_products, mesh=fine, in_specs=in_specs, out_specs=out_specs, check_vma=False)
```

```python
import functools

import jax
import jax.numpy as jnp
from jax import lax
from jax.experimental import pallas as pl
from jax.experimental.pallas import tpu as pltpu
from jax.sharding import Mesh
from jax.sharding import PartitionSpec as P

LINE = ("zh", "zl")
PAIR_LINE = ("c", "zh", "zl")
NT = (((1,), (1,)), ((), ()))
TN = (((0,), (0,)), ((), ()))


def turned(x, steps):
    pairs = [
        (c * 16 + z, c * 16 + (z + (steps if c == 0 else -steps)) % 16)
        for c in range(2)
        for z in range(16)
    ]
    return lax.ppermute(x, PAIR_LINE, pairs)


def forward_kernel(at, own, ahead, back, two, v0, v1, u0, u1, out, coeffs):
    for k, v in enumerate((v0, v1)):
        side = jnp.bitwise_xor(at[0], k)
        for j in range(4):
            cols = pl.ds(j * 512, 512)
            x = jnp.concatenate([piece[side, :, cols] for piece in (own, ahead, back, two)], 0)
            tall = jnp.concatenate([v[i, j] for i in range(4)], 0)
            c = lax.dot_general(tall, x, NT, preferred_element_type=jnp.float32)
            for i in range(4):
                coeffs[i, pl.ds(k * 320 + j * 80, 80), :] = c[i * 80 : i * 80 + 80].astype(jnp.bfloat16)
    for i in range(4):
        u = jnp.concatenate([u[i, j] for u in (u0, u1) for j in range(4)], 0)
        part = lax.dot_general(coeffs[i], u, TN, preferred_element_type=jnp.float32)
        for p in range(4):
            for zh in range(4):
                row = p * 32 + zh * 8
                out[zh * 4 + at[1 + p], :, pl.ds(i * 512, 512)] = part[row : row + 8].astype(jnp.bfloat16)


def adjoint_kernel(at, w, v0, v1, u0, u1, own, ahead, back, two, coeffs, blocks):
    for k, u in enumerate((u0, u1)):
        for i in range(4):
            tall = jnp.concatenate([u[i, j] for j in range(4)], 0)
            a = lax.dot_general(tall, w[:, pl.ds(i * 512, 512)], NT, preferred_element_type=jnp.float32)
            for j in range(4):
                coeffs[k, j, pl.ds(i * 80, 80), :] = a[j * 80 : j * 80 + 80].astype(jnp.bfloat16)
    for k, v in enumerate((v0, v1)):
        side = jnp.bitwise_xor(at[0], k)
        for j in range(4):
            tall = jnp.concatenate([v[i, j] for i in range(4)], 0)
            block = lax.dot_general(coeffs[k, j], tall, TN, preferred_element_type=jnp.float32)
            block = block.astype(jnp.bfloat16)
            for q in range(4):
                blocks[q, side, j] = block[:, q * 128 : q * 128 + 128]
    own[...] = blocks[at[1]]
    back[...] = blocks[at[2]]
    ahead[...] = blocks[at[3]]
    two[...] = blocks[at[4]]


SMEM = pl.BlockSpec(memory_space=pltpu.SMEM)
VMEM = pl.BlockSpec(memory_space=pltpu.VMEM)
ROOM = pltpu.CompilerParams(vmem_limit_bytes=20 * 1024 * 1024)


def forward_part(at, pieces, v, u):
    return pl.pallas_call(
        forward_kernel,
        out_shape=jax.ShapeDtypeStruct((16, 8, 2048), jnp.bfloat16),
        in_specs=[SMEM] + [VMEM] * 8,
        out_specs=VMEM,
        scratch_shapes=[pltpu.VMEM((4, 640, 128), jnp.bfloat16)],
        compiler_params=ROOM,
        name="forward_part",
    )(at, *pieces, *v, *u)


def adjoint_part(at, weighted, v, u):
    blocks = jax.ShapeDtypeStruct((2, 4, 128, 128), jnp.bfloat16)
    return pl.pallas_call(
        adjoint_kernel,
        out_shape=(blocks,) * 4,
        in_specs=[SMEM] + [VMEM] * 5,
        out_specs=(VMEM,) * 4,
        scratch_shapes=[
            pltpu.VMEM((2, 4, 320, 128), jnp.bfloat16),
            pltpu.VMEM((4, 2, 4, 128, 128), jnp.bfloat16),
        ],
        compiler_params=ROOM,
        name="adjoint_part",
    )(at, weighted, *v, *u)


def exchange(blocks, axes):
    return lax.all_to_all(blocks, axes, split_axis=0, concat_axis=0, tiled=True)


def wide(x):
    return x.astype(jnp.float32)


def both_products(samples, row_weights, tile_ranks, u_factors, v_factors):
    core = lax.axis_index("c")
    place = lax.axis_index("zl")
    turn = 1 - 2 * core
    swap = functools.partial(lax.ppermute, axis_name="c", perm=[(0, 1), (1, 0)])
    at = jnp.stack([core, place, (place - turn) & 3, (place + turn) & 3, (place + 2) & 3]).astype(jnp.int32)

    x = samples.astype(jnp.bfloat16).reshape(2, 1, 8, 2048)
    x = jnp.broadcast_to(x, (2, 4, 8, 2048)).reshape(8, 8, 2048)
    far = exchange(x, ("c", "zh")).reshape(2, 32, 2048)
    levels = lax.broadcasted_iota(jnp.int32, (1, 1, 80, 1), 2)
    ranked = jnp.where(levels < tile_ranks[:, :, None, None], u_factors, jnp.zeros_like(u_factors))
    v = (v_factors, swap(v_factors))
    u = (ranked, swap(ranked))

    two = turned(far, 2)
    ahead = turned(far, 1)
    back = turned(far, -1)
    part = forward_part(at, (far, ahead, back, two), v, u)
    forward_rows = jnp.sum(wide(exchange(part, ("xy",))), axis=0)

    weighted = (forward_rows * row_weights[None, :]).astype(jnp.bfloat16)
    weighted = exchange(jnp.broadcast_to(weighted, (16, 8, 2048)), ("xy",)).reshape(128, 2048)

    own, ahead, back, two = adjoint_part(at, weighted, v, u)
    two = turned(two, 2)
    ahead = turned(ahead, 1)
    back = turned(back, -1)
    near = wide(own) + wide(ahead) + wide(back) + wide(two)
    near = near.astype(jnp.bfloat16).reshape(8, 128, 128)
    blocks = exchange(near, ("c", "zh")).reshape(2, 4, 16, 8, 128)
    blocks = jnp.sum(wide(blocks), axis=1)
    adjoint_cols = jnp.swapaxes(blocks, 0, 1).reshape(256, 128)
    return forward_rows, adjoint_cols


def solution(mesh):
    fine = Mesh(mesh.devices.reshape(16, 2, 4, 4), ("xy", "c", "zh", "zl"))
    narrow, wide_axes = LINE, ("xy", "c")
    in_specs = (
        P(narrow, wide_axes),
        P(narrow),
        P(narrow, wide_axes),
        P(narrow, wide_axes, None, None),
        P(narrow, wide_axes, None, None),
    )
    out_specs = (P(wide_axes, narrow), P(None, (*wide_axes, *narrow)))
    return jax.shard_map(both_products, mesh=fine, in_specs=in_specs, out_specs=out_specs, check_vma=False)
```

```python
import functools

import jax
import jax.numpy as jnp
from jax import lax
from jax.experimental import pallas as pl
from jax.experimental.pallas import tpu as pltpu
from jax.sharding import Mesh
from jax.sharding import PartitionSpec as P

LINE = ("zh", "zl")
PAIR_LINE = ("c", "zh", "zl")
NT = (((1,), (1,)), ((), ()))
TN = (((0,), (0,)), ((), ()))


def turned(x, steps):
    pairs = [
        (c * 16 + z, c * 16 + (z + (steps if c == 0 else -steps)) % 16)
        for c in range(2)
        for z in range(16)
    ]
    return lax.ppermute(x, PAIR_LINE, pairs)


def coeffs_kernel(own, ahead, back, two, v0, v1, coeffs):
    for k, v in enumerate((v0, v1)):
        for j in range(4):
            cols = pl.ds(k * 2048 + j * 512, 512)
            x = jnp.concatenate([piece[:, cols] for piece in (own, ahead, back, two)], 0)
            tall = jnp.concatenate([v[i, j] for i in range(4)], 0)
            c = lax.dot_general(tall, x, NT, preferred_element_type=jnp.float32)
            for i in range(4):
                coeffs[i, pl.ds(k * 320 + j * 80, 80), :] = c[i * 80 : i * 80 + 80].astype(jnp.bfloat16)


def forward_kernel(at, coeffs, u0, u1, out):
    for i in range(4):
        u = jnp.concatenate([u[i, j] for u in (u0, u1) for j in range(4)], 0)
        part = lax.dot_general(coeffs[i], u, TN, preferred_element_type=jnp.float32)
        for p in range(4):
            for zh in range(4):
                row = p * 32 + zh * 8
                out[zh * 4 + at[1 + p], :, pl.ds(i * 512, 512)] = part[row : row + 8].astype(jnp.bfloat16)


def adjoint_kernel(at, w, v0, v1, u0, u1, own, ahead, back, two, coeffs, blocks):
    for k, u in enumerate((u0, u1)):
        for i in range(4):
            tall = jnp.concatenate([u[i, j] for j in range(4)], 0)
            a = lax.dot_general(tall, w[:, pl.ds(i * 512, 512)], NT, preferred_element_type=jnp.float32)
            for j in range(4):
                coeffs[k, j, pl.ds(i * 80, 80), :] = a[j * 80 : j * 80 + 80].astype(jnp.bfloat16)
    for k, v in enumerate((v0, v1)):
        side = jnp.bitwise_xor(at[0], k)
        for j in range(4):
            tall = jnp.concatenate([v[i, j] for i in range(4)], 0)
            block = lax.dot_general(coeffs[k, j], tall, TN, preferred_element_type=jnp.float32)
            block = block.astype(jnp.bfloat16)
            for q in range(4):
                blocks[q, side, j] = block[:, q * 128 : q * 128 + 128]
    own[...] = blocks[at[1]]
    back[...] = blocks[at[2]]
    ahead[...] = blocks[at[3]]
    two[...] = blocks[at[4]]


SMEM = pl.BlockSpec(memory_space=pltpu.SMEM)
VMEM = pl.BlockSpec(memory_space=pltpu.VMEM)
ROOM = pltpu.CompilerParams(vmem_limit_bytes=20 * 1024 * 1024)


def forward_part(at, pieces, v, u):
    coeffs = pl.pallas_call(
        coeffs_kernel,
        out_shape=jax.ShapeDtypeStruct((4, 640, 128), jnp.bfloat16),
        in_specs=[VMEM] * 6,
        out_specs=VMEM,
        compiler_params=ROOM,
        name="forward_coeffs",
    )(*pieces, *v)
    return pl.pallas_call(
        forward_kernel,
        out_shape=jax.ShapeDtypeStruct((16, 8, 2048), jnp.bfloat16),
        in_specs=[SMEM] + [VMEM] * 3,
        out_specs=VMEM,
        compiler_params=ROOM,
        name="forward_part",
    )(at, coeffs, *u)


def adjoint_part(at, weighted, v, u):
    blocks = jax.ShapeDtypeStruct((2, 4, 128, 128), jnp.bfloat16)
    return pl.pallas_call(
        adjoint_kernel,
        out_shape=(blocks,) * 4,
        in_specs=[SMEM] + [VMEM] * 5,
        out_specs=(VMEM,) * 4,
        scratch_shapes=[
            pltpu.VMEM((2, 4, 320, 128), jnp.bfloat16),
            pltpu.VMEM((4, 2, 4, 128, 128), jnp.bfloat16),
        ],
        compiler_params=ROOM,
        name="adjoint_part",
    )(at, weighted, *v, *u)


def exchange(blocks, axes):
    return lax.all_to_all(blocks, axes, split_axis=0, concat_axis=0, tiled=True)


def wide(x):
    return x.astype(jnp.float32)


def both_products(samples, row_weights, tile_ranks, u_factors, v_factors):
    core = lax.axis_index("c")
    place = lax.axis_index("zl")
    turn = 1 - 2 * core
    swap = functools.partial(lax.ppermute, axis_name="c", perm=[(0, 1), (1, 0)])
    at = jnp.stack([core, place, (place - turn) & 3, (place + turn) & 3, (place + 2) & 3]).astype(jnp.int32)

    x = samples.astype(jnp.bfloat16).reshape(2, 8, 2048)
    kept = lax.dynamic_index_in_dim(x, core, 0, keepdims=False)
    given = lax.dynamic_index_in_dim(x, 1 - core, 0, keepdims=False)
    block = jnp.concatenate([kept, swap(given)], 1)
    far = lax.all_gather(block, "zh", axis=0, tiled=True)
    far, u_factors, v_factors = lax.optimization_barrier((far, u_factors, v_factors))
    two = turned(far, 2)
    ahead = turned(far, 1)
    back = turned(far, -1)
    levels = lax.broadcasted_iota(jnp.int32, (1, 1, 80, 1), 2)
    ranked = jnp.where(levels < tile_ranks[:, :, None, None], u_factors, jnp.zeros_like(u_factors))
    v = (v_factors, swap(v_factors))
    u = (ranked, swap(ranked))
    part = forward_part(at, (far, ahead, back, two), v, u)
    forward_rows = jnp.sum(wide(exchange(part, ("xy",))), axis=0)

    weighted = (forward_rows * row_weights[None, :]).astype(jnp.bfloat16)
    weighted = exchange(jnp.broadcast_to(weighted, (16, 8, 2048)), ("xy",)).reshape(128, 2048)

    own, ahead, back, two = adjoint_part(at, weighted, v, u)
    two = turned(two, 2)
    ahead = turned(ahead, 1)
    back = turned(back, -1)
    near = wide(own) + wide(ahead) + wide(back) + wide(two)
    near = near.astype(jnp.bfloat16).reshape(8, 128, 128)
    blocks = exchange(near, ("c", "zh")).reshape(2, 4, 16, 8, 128)
    blocks = jnp.sum(wide(blocks), axis=1)
    adjoint_cols = jnp.swapaxes(blocks, 0, 1).reshape(256, 128)
    return forward_rows, adjoint_cols


def solution(mesh):
    fine = Mesh(mesh.devices.reshape(16, 2, 4, 4), ("xy", "c", "zh", "zl"))
    narrow, wide_axes = LINE, ("xy", "c")
    in_specs = (
        P(narrow, wide_axes),
        P(narrow),
        P(narrow, wide_axes),
        P(narrow, wide_axes, None, None),
        P(narrow, wide_axes, None, None),
    )
    out_specs = (P(wide_axes, narrow), P(None, (*wide_axes, *narrow)))
    return jax.shard_map(both_products, mesh=fine, in_specs=in_specs, out_specs=out_specs, check_vma=False)
```

```python
import functools

import jax
import jax.numpy as jnp
from jax import lax
from jax.experimental import pallas as pl
from jax.experimental.pallas import tpu as pltpu
from jax.sharding import Mesh
from jax.sharding import PartitionSpec as P

LINE = ("zh", "zl")
PAIR_LINE = ("c", "zh", "zl")
NT = (((1,), (1,)), ((), ()))
TN = (((0,), (0,)), ((), ()))


def turned(x, steps):
    pairs = [
        (c * 16 + z, c * 16 + (z + (steps if c == 0 else -steps)) % 16)
        for c in range(2)
        for z in range(16)
    ]
    return lax.ppermute(x, PAIR_LINE, pairs)


def coeffs_kernel(own, ahead, back, two, v0, v1, coeffs):
    for k, v in enumerate((v0, v1)):
        for j in range(4):
            cols = pl.ds(k * 2048 + j * 512, 512)
            x = jnp.concatenate([piece[:, cols] for piece in (own, ahead, back, two)], 0)
            tall = jnp.concatenate([v[i, j] for i in range(4)], 0)
            c = lax.dot_general(tall, x, NT, preferred_element_type=jnp.float32)
            for i in range(4):
                coeffs[i, pl.ds(k * 320 + j * 80, 80), :] = c[i * 80 : i * 80 + 80].astype(jnp.bfloat16)


def forward_kernel(at, coeffs, u0, u1, out):
    for i in range(4):
        u = jnp.concatenate([u[i, j] for u in (u0, u1) for j in range(4)], 0)
        part = lax.dot_general(coeffs[i], u, TN, preferred_element_type=jnp.float32)
        for p in range(4):
            for zh in range(4):
                row = p * 32 + zh * 8
                out[zh * 4 + at[1 + p], :, pl.ds(i * 512, 512)] = part[row : row + 8].astype(jnp.bfloat16)


def adjoint_kernel(at, w, v0, v1, u0, u1, coeffs, ahead, back, two):
    for k, u in enumerate((u0, u1)):
        for i in range(4):
            tall = jnp.concatenate([u[i, j] for j in range(4)], 0)
            a = lax.dot_general(tall, w[:, pl.ds(i * 512, 512)], NT, preferred_element_type=jnp.float32)
            for j in range(4):
                coeffs[k, j, pl.ds(i * 80, 80), :] = a[j * 80 : j * 80 + 80].astype(jnp.bfloat16)
    for place, block in ((at[4], two), (at[3], ahead), (at[2], back)):
        place_blocks(at[0], place, coeffs, v0, v1, block)


def own_kernel(at, coeffs, v0, v1, own):
    place_blocks(at[0], at[1], coeffs, v0, v1, own)


def place_blocks(core, place, coeffs, v0, v1, block):
    cols = pl.ds(pl.multiple_of(place * 128, 128), 128)
    for k, v in enumerate((v0, v1)):
        side = jnp.bitwise_xor(core, k)
        for j in range(4):
            tall = jnp.concatenate([v[i, j, :, cols] for i in range(4)], 0)
            part = lax.dot_general(coeffs[k, j], tall, TN, preferred_element_type=jnp.float32)
            block[side, j] = part.astype(jnp.bfloat16)


SMEM = pl.BlockSpec(memory_space=pltpu.SMEM)
VMEM = pl.BlockSpec(memory_space=pltpu.VMEM)
ROOM = pltpu.CompilerParams(vmem_limit_bytes=20 * 1024 * 1024)


def forward_part(at, pieces, v, u):
    coeffs = pl.pallas_call(
        coeffs_kernel,
        out_shape=jax.ShapeDtypeStruct((4, 640, 128), jnp.bfloat16),
        in_specs=[VMEM] * 6,
        out_specs=VMEM,
        compiler_params=ROOM,
        name="forward_coeffs",
    )(*pieces, *v)
    return pl.pallas_call(
        forward_kernel,
        out_shape=jax.ShapeDtypeStruct((16, 8, 2048), jnp.bfloat16),
        in_specs=[SMEM] + [VMEM] * 3,
        out_specs=VMEM,
        compiler_params=ROOM,
        name="forward_part",
    )(at, coeffs, *u)


def adjoint_part(at, weighted, v, u):
    blocks = jax.ShapeDtypeStruct((2, 4, 128, 128), jnp.bfloat16)
    coeffs, ahead, back, two = pl.pallas_call(
        adjoint_kernel,
        out_shape=(jax.ShapeDtypeStruct((2, 4, 320, 128), jnp.bfloat16),) + (blocks,) * 3,
        in_specs=[SMEM] + [VMEM] * 5,
        out_specs=(VMEM,) * 4,
        compiler_params=ROOM,
        name="adjoint_part",
    )(at, weighted, *v, *u)
    own = pl.pallas_call(
        own_kernel,
        out_shape=blocks,
        in_specs=[SMEM] + [VMEM] * 3,
        out_specs=VMEM,
        compiler_params=ROOM,
        name="own_part",
    )(at, coeffs, *v)
    return own, ahead, back, two


def exchange(blocks, axes):
    return lax.all_to_all(blocks, axes, split_axis=0, concat_axis=0, tiled=True)


def wide(x):
    return x.astype(jnp.float32)


def both_products(samples, row_weights, tile_ranks, u_factors, v_factors):
    core = lax.axis_index("c")
    place = lax.axis_index("zl")
    turn = 1 - 2 * core
    swap = functools.partial(lax.ppermute, axis_name="c", perm=[(0, 1), (1, 0)])
    at = jnp.stack([core, place, (place - turn) & 3, (place + turn) & 3, (place + 2) & 3]).astype(jnp.int32)

    x = samples.astype(jnp.bfloat16).reshape(2, 8, 2048)
    kept = lax.dynamic_index_in_dim(x, core, 0, keepdims=False)
    given = lax.dynamic_index_in_dim(x, 1 - core, 0, keepdims=False)
    block = jnp.concatenate([kept, swap(given)], 1)
    far = lax.all_gather(block, "zh", axis=0, tiled=True)
    far, u_factors, v_factors = lax.optimization_barrier((far, u_factors, v_factors))
    two = turned(far, 2)
    ahead = turned(far, 1)
    back = turned(far, -1)
    kept_ranks = lax.broadcasted_iota(jnp.int32, (4, 4, 80), 2) < tile_ranks[:, :, None]
    ranked = jnp.where(kept_ranks[..., None], u_factors, jnp.zeros_like(u_factors))
    v = (v_factors, swap(v_factors))
    u = (ranked, swap(ranked))
    part = forward_part(at, (far, ahead, back, two), v, u)
    forward_rows = jnp.sum(wide(exchange(part, ("xy",))), axis=0)

    weighted = (forward_rows * row_weights[None, :]).astype(jnp.bfloat16)
    weighted = exchange(jnp.broadcast_to(weighted, (16, 8, 2048)), ("xy",)).reshape(128, 2048)

    own, ahead, back, two = adjoint_part(at, weighted, v, u)
    two = turned(two, 2)
    ahead = turned(ahead, 1)
    back = turned(back, -1)
    near = wide(own) + wide(ahead) + wide(back) + wide(two)
    near = near.astype(jnp.bfloat16).reshape(8, 128, 128)
    blocks = exchange(near, ("c", "zh")).reshape(2, 4, 16, 8, 128)
    blocks = jnp.sum(wide(blocks), axis=1)
    adjoint_cols = jnp.swapaxes(blocks, 0, 1).reshape(256, 128)
    return forward_rows, adjoint_cols


def solution(mesh):
    fine = Mesh(mesh.devices.reshape(16, 2, 4, 4), ("xy", "c", "zh", "zl"))
    narrow, wide_axes = LINE, ("xy", "c")
    in_specs = (
        P(narrow, wide_axes),
        P(narrow),
        P(narrow, wide_axes),
        P(narrow, wide_axes, None, None),
        P(narrow, wide_axes, None, None),
    )
    out_specs = (P(wide_axes, narrow), P(None, (*wide_axes, *narrow)))
    return jax.shard_map(both_products, mesh=fine, in_specs=in_specs, out_specs=out_specs, check_vma=False)
```
